32 devices in a mesh: rows: 4 (over y, x), cols: 2 (over core), slabs: 4 (over z).
Axes of the slice: x: 2, y: 2, z: 4, core: 2. Of those that a mesh axis runs over, the one named last changes fastest.
Arguments:
- field_values: float32 [16, 64, 512, 128], P('rows', 'cols', 'slabs'), may hold values from 0.5 to 2
- mobility: float32 [16, 64, 512, 128], P('rows', 'cols', 'slabs'), may hold values from 0.03 to 0.15
- source: float32 [16, 64, 512, 128], P('rows', 'cols', 'slabs'), may hold values from -0.2 to 0.2
Outputs:
- anomaly: float32 [16, 64, 512, 128], P('rows', 'cols', 'slabs')
- field_values_end: float32 [16, 64, 512, 128], P('rows', 'cols', 'slabs')
The draws below stay inside these ranges and needn't reach their ends.
All inputs are finite; a program needn't handle non-finite values.
Results may differ from the reference program's by a relative error of at most 0.00002.
Values sent between devices are 32-bit elements; how exact they have to be, the bound alone decides.
No kernel may reach another device: no remote copies, remote signals or barrier semaphores. Data moves between devices by JAX's collectives and lax.ppermute only.
A program may use at most 128 MiB of HBM per device.

```python
import jax
import jax.numpy as jnp
from jax import lax

GRID_Y = 16
GRID_X = 64
GRID_Z = 512
LEVELS = 128
STEPS = 3


def shard_levels(stream_key, shape, split, least, largest):
    factor_of = 1.0
    for axis_at, shards_of in split:
        steps = jax.random.uniform(jax.random.fold_in(jax.random.fold_in(stream_key, 6), axis_at), (shards_of,), jnp.float32, least / len(split), largest / len(split))
        factor_of = factor_of * jnp.repeat(jnp.exp(steps), shape[axis_at] // shards_of).reshape((-1,) + (1,) * (len(shape) - 1 - axis_at))
    return factor_of


def setup_inputs(seed: int = 0) -> dict:
    splits = jax.random.split(jax.random.key(seed), 4)
    return {
        "field_values": jnp.clip(0.5 + 1.5 * jax.random.uniform(splits[0], (GRID_Y, GRID_X, GRID_Z, LEVELS), jnp.float32) ** shard_levels(splits[0], (GRID_Y, GRID_X, GRID_Z, LEVELS), ((0, 4), (1, 2), (2, 4)), -0.2, 0.2), 0.5, 2.0),
        "mobility": jnp.clip(0.03 + 0.120000007 * jax.random.uniform(splits[1], (GRID_Y, GRID_X, GRID_Z, LEVELS), jnp.float32) ** shard_levels(splits[1], (GRID_Y, GRID_X, GRID_Z, LEVELS), ((0, 4), (1, 2), (2, 4)), -0.2, 0.2), 0.03, 0.15),
        "source": jnp.clip(jax.random.uniform(splits[2], (GRID_Y, GRID_X, GRID_Z, LEVELS), jnp.float32, -0.2, 0.2) * shard_levels(splits[2], (GRID_Y, GRID_X, GRID_Z, LEVELS), ((0, 4), (1, 2), (2, 4)), -0.4, 0.0), -0.2, 0.2),
    }


def strip_edges(values, dims):
    for dim in dims:
        values = lax.slice_in_dim(values, 1, values.shape[dim] - 1, axis=dim)
    return values

def neighbour(values, dim, start, dims):
    others = [other for other in dims if other != dim]
    values = strip_edges(values, others)
    return lax.slice_in_dim(values, start, start + values.shape[dim] - 2, axis=dim)

def one_step(padded, mobility, source):
    middle = strip_edges(padded, (0, 1, 2))
    lower = [neighbour(padded, dim, 0, (0, 1, 2)) for dim in (0, 1, 2)]
    upper = [neighbour(padded, dim, 2, (0, 1, 2)) for dim in (0, 1, 2)]
    spread = lower[0] + upper[0] + lower[1] + upper[1] + lower[2] + upper[2] - 6.0 * middle
    return middle + mobility * spread + source

def reference(field_values, mobility, source):
    for step in range(STEPS):
        field_values = one_step(jnp.pad(field_values, ((1, 1), (1, 1), (1, 1), (0, 0)), mode='wrap'), mobility, source)
    line_mean = lax.optimization_barrier(jnp.mean(field_values, axis=2, keepdims=True))
    centred = field_values - line_mean
    line_variance = lax.optimization_barrier(jnp.mean(centred * centred, axis=2, keepdims=True))
    anomaly = centred * lax.rsqrt(line_variance + 0.0001)
    return (anomaly, field_values)
```

```python
import functools

import jax
import jax.numpy as jnp
from jax import lax
from jax.experimental import pallas as pl
from jax.experimental.pallas import tpu as pltpu
from jax.sharding import PartitionSpec as P

STEPS = 3
EPSILON = 0.0001
HEAD = 8
TAIL = 16
VMEM_BYTES = 12 * 2**20
OUTPUTS = {"step": 3, "last": 3, "partial": 2}


def ring(axis, shift):
    count = lax.axis_size(axis)
    return [(i, (i + shift) % count) for i in range(count)]


def shifted(block, axis, shift):
    return lax.ppermute(block, axis, ring(axis, shift))


def rows_per_block(*sizes):
    for rows in (8, 4, 2):
        if all(size % rows == 0 for size in sizes):
            return rows
    return 1


def plane_spec(source, rows, start):
    if isinstance(source, tuple):
        array, plane = source
        return array, pl.BlockSpec((None, rows) + array.shape[2:], lambda i: (plane, start(i), 0, 0))
    return source, pl.BlockSpec((rows,) + source.shape[1:], lambda i: (start(i), 0, 0))


def call(body, grid, specs, out_specs, out_shape, aliases, flops):
    bytes_accessed = sum(4 * s.size for s in out_shape)
    return pl.pallas_call(
        body,
        grid=grid,
        in_specs=[spec for _, spec in specs],
        out_specs=out_specs,
        out_shape=out_shape,
        input_output_aliases=aliases,
        cost_estimate=pl.CostEstimate(flops=flops, bytes_accessed=bytes_accessed, transcendentals=0),
        compiler_params=pltpu.CompilerParams(vmem_limit_bytes=VMEM_BYTES),
    )(*[array for array, _ in specs])


def token_spec():
    return jax.ShapeDtypeStruct((8, 128), jnp.float32), pl.BlockSpec((8, 128), lambda i: (0, 0))


def anywhere(arrays):
    return [(array, pl.BlockSpec(memory_space=pl.ANY)) for array in arrays]


def stencil_row(j, rows, sides, refs):
    center, before, after, mobility, source, x_low, x_high, z_low, z_high = refs
    i = pl.program_id(0)
    last = pl.num_programs(0) - 1
    middle = center[j]
    depth = middle.shape[0]
    left = center[j - 1] if j > 0 else jnp.where(i == 0, x_low[...], before[0])
    right = center[j + 1] if j < rows - 1 else jnp.where(i == last, x_high[...], after[0])
    z = lax.broadcasted_iota(jnp.int32, middle.shape, 0)
    lower = jnp.where(z == 0, z_low[j : j + 1, :], pltpu.roll(middle, 1, 0))
    upper = jnp.where(z == depth - 1, z_high[j : j + 1, :], pltpu.roll(middle, depth - 1, 0))
    spread = left + right + lower + upper - 6.0 * middle
    for side in sides:
        spread = spread + side[j]
    return middle + mobility[j] * spread + source[j]


def write_stats(stats, j, value):
    mean = jnp.sum(value, axis=0, keepdims=True) * (1.0 / value.shape[0])
    off = value - mean
    stats[0, j : j + 1, :] = mean
    stats[1, j : j + 1, :] = jnp.sum(off * off, axis=0, keepdims=True)


def update_body(*refs, rows, sides, kind):
    beside, ins = refs[:sides], refs[sides : sides + 9]
    outs = refs[-OUTPUTS[kind] :]
    for j in range(rows):
        value = stencil_row(j, rows, beside, ins)
        outs[0][j] = value
        if kind == "step":
            outs[1][j : j + 1, :] = value[:1]
            outs[2][j : j + 1, :] = value[-1:]
        if kind == "last":
            write_stats(outs[1], j, value)
            outs[2][j] = value
        if kind == "partial":
            outs[1][j] = ins[3][j]


def update(plane, sides, center, mobility, source, x_halo, z_halo, kind, end=()):
    size, depth, levels = mobility.shape[1:]
    rows = rows_per_block(size)
    same = lambda i: i
    specs = [plane_spec(side, rows, same) for side in sides]
    specs += [
        plane_spec(center, rows, same),
        plane_spec(center, 1, lambda i: jnp.maximum(i * rows - 1, 0)),
        plane_spec(center, 1, lambda i: jnp.minimum(i * rows + rows, size - 1)),
        plane_spec((mobility, plane), rows, same),
        plane_spec((source, plane), rows, same),
    ]
    specs += [(h, pl.BlockSpec((None, depth, levels), lambda i: (plane, 0, 0))) for h in x_halo]
    specs += [(h, pl.BlockSpec((None, rows, levels), lambda i: (plane, i, 0))) for h in z_halo]
    out_shape = [jax.ShapeDtypeStruct((size, depth, levels), jnp.float32)]
    out_specs = [pl.BlockSpec((rows, depth, levels), lambda i: (i, 0, 0))]
    aliases = {}
    if kind == "partial":
        out_shape, out_specs = out_shape * 2, out_specs * 2
    if kind == "last":
        out_shape += [jax.ShapeDtypeStruct((2, size, levels), jnp.float32)]
        out_specs += [pl.BlockSpec((2, rows, levels), lambda i: (0, i, 0))]
        out_shape += [jax.ShapeDtypeStruct(mobility.shape, jnp.float32)]
        out_specs += [pl.BlockSpec((None, rows, depth, levels), lambda i: (plane, i, 0, 0))]
        aliases = {len(specs) + k: 2 for k in range(len(end))}
        specs += anywhere(end)
    if kind == "step":
        out_shape += [jax.ShapeDtypeStruct((size, levels), jnp.float32)] * 2
        out_specs += [pl.BlockSpec((rows, levels), lambda i: (i, 0))] * 2
    body = functools.partial(update_body, rows=rows, sides=len(sides), kind=kind)
    return call(body, (size // rows,), specs, out_specs, out_shape, aliases, 20 * size * depth * levels)


def finish_body(*refs, rows):
    partial, mobility, side = refs[:3]
    out, stats = refs[-2:]
    for j in range(rows):
        value = partial[j] + mobility[j] * side[j]
        out[j] = value
        write_stats(stats, j, value)


def finish(start, partial, mobility, side, after):
    size, depth, levels = side.shape
    rows = rows_per_block(size, start)
    first = start // rows
    specs = [
        plane_spec(partial, rows, lambda i: first + i),
        plane_spec(mobility, rows, lambda i: first + i),
        plane_spec(side, rows, lambda i: i),
    ]
    specs += anywhere(after)
    out_shape = [
        jax.ShapeDtypeStruct((size, depth, levels), jnp.float32),
        jax.ShapeDtypeStruct((2, size, levels), jnp.float32),
    ]
    out_specs = [
        pl.BlockSpec((rows, depth, levels), lambda i: (i, 0, 0)),
        pl.BlockSpec((2, rows, levels), lambda i: (0, i, 0)),
    ]
    body = functools.partial(finish_body, rows=rows)
    return call(body, (size // rows,), specs, out_specs, out_shape, {}, 8 * size * depth * levels)


def scale_body(*refs, slabs):
    field, stats = refs[0], refs[1 : 1 + slabs]
    anomaly, token = refs[-2:]
    token[...] = jnp.zeros_like(token)
    rows, depth = field.shape[:2]
    mean = sum(s[0] for s in stats) * (1.0 / slabs)
    total = sum(s[1] for s in stats)
    for s in stats:
        off = s[0] - mean
        total = total + depth * (off * off)
    scale = lax.rsqrt(total * (1.0 / (depth * slabs)) + EPSILON)
    for j in range(rows):
        anomaly[j] = (field[j] - mean[j : j + 1, :]) * scale[j : j + 1, :]


def gathered(stats):
    parts = [stats]
    for shift in range(1, lax.axis_size("slabs")):
        parts.append(shifted(stats, "slabs", shift))
    return parts


def store_body(source, *refs):
    refs[-1][...] = source[...]


def stored(plane, start, whole, field, outs):
    size, depth, levels = field.shape
    rows = rows_per_block(size, start)
    first = start // rows
    specs = [plane_spec(field, rows, lambda i: i)] + anywhere(outs)
    out_specs = [pl.BlockSpec((None, rows, depth, levels), lambda i: (plane, first + i, 0, 0))]
    out_shape = [jax.ShapeDtypeStruct(whole, jnp.float32)]
    aliases = {1 + k: k for k in range(len(outs))}
    return call(store_body, (size // rows,), specs, out_specs, out_shape, aliases, 0)


def scaled(plane, start, whole, field, stats, outs):
    size, depth, levels = field.shape
    rows = rows_per_block(size, start)
    first = start // rows
    slabs = len(stats)
    specs = [plane_spec(field, rows, lambda i: i)]
    specs += [(s, pl.BlockSpec((2, rows, levels), lambda i: (0, i, 0))) for s in stats]
    specs += anywhere(outs)
    token_shape, token = token_spec()
    out_specs = [pl.BlockSpec((None, rows, depth, levels), lambda i: (plane, first + i, 0, 0)), token]
    out_shape = [jax.ShapeDtypeStruct(whole, jnp.float32), token_shape]
    aliases = {1 + slabs + k: k for k in range(len(outs))}
    body = functools.partial(scale_body, slabs=slabs)
    return call(body, (size // rows,), specs, out_specs, out_shape, aliases, 4 * size * depth * levels)


def copy_body(source, *refs, plane, start):
    pltpu.sync_copy(source.at[plane, pl.ds(start, refs[-2].shape[0])], refs[-2])
    refs[-1][...] = jnp.zeros_like(refs[-1])


def copied(array, plane, start, size, after):
    token_shape, _ = token_spec()
    specs = [(array, pl.BlockSpec(memory_space=pltpu.HBM))] + anywhere(after)
    out_shape = [jax.ShapeDtypeStruct((size,) + array.shape[2:], jnp.float32), token_shape]
    out_specs = [pl.BlockSpec(memory_space=pltpu.VMEM)] * 2
    body = functools.partial(copy_body, plane=plane, start=start)
    return call(body, (), specs, out_specs, out_shape, {}, 0)


def per_device(field, mobility, source):
    planes, size, depth, _ = field.shape
    top = planes - 1
    edges = field
    field, mobility, source = (pltpu.with_memory_space_constraint(a, pltpu.HBM) for a in (field, mobility, source))
    now = [(field, p) for p in range(planes)]
    head = HEAD if size > HEAD else 0
    opening = []
    token = ()
    for start, stop in ((0, head), (head, size)):
        if start < stop:
            part, *token = copied(field, top, start, stop - start, token)
            opening.append(shifted(part, "rows", 1))
    up = jnp.concatenate(opening) if head else opening[0]
    lows, _ = copied(field, 0, 0, size, token)
    down = shifted(lows, "rows", -1)
    x_edges = (edges[:, size - 1], edges[:, 0])
    z_edges = (edges[:, :, depth - 1], edges[:, :, 0])
    for step in range(STEPS - 1):
        x_halo = (shifted(x_edges[0], "cols", 1), shifted(x_edges[1], "cols", -1))
        z_halo = (shifted(z_edges[0], "slabs", 1), shifted(z_edges[1], "slabs", -1))
        new = {}
        order = [0, top] if step % 2 == 0 else [top, 0]
        for p in list(range(1, top)) + order:
            sides = (up if p == 0 else now[p - 1], down if p == top else now[p + 1])
            new[p] = update(p, sides, now[p], mobility, source, x_halo, z_halo, "step")
        cut = size - TAIL if step == STEPS - 2 else size
        sent = {}
        for p in order:
            value = new[p][0]
            parts = [value] if cut == size or p == order[0] else [value[:cut], value[cut:]]
            sent[p] = [shifted(part, "rows", -1 if p == 0 else 1) for part in parts]
        if cut == size:
            down, up = sent[0][0], sent[top][0]
        now = [new[p][0] for p in range(planes)]
        x_edges = (jnp.stack([v[size - 1] for v in now]), jnp.stack([v[0] for v in now]))
        z_edges = tuple(jnp.stack([new[p][k] for p in range(planes)]) for k in (2, 1))

    x_halo = (shifted(x_edges[0], "cols", 1), shifted(x_edges[1], "cols", -1))
    z_halo = (shifted(z_edges[0], "slabs", 1), shifted(z_edges[1], "slabs", -1))
    early, late = (top, 0) if STEPS % 2 == 0 else (0, top)
    outs, end = (), ()
    for p in list(range(1, top)) + [early]:
        sides = [now[q] for q in (p - 1, p + 1) if 0 <= q <= top]
        sides += sent[order[0]] if p == early else []
        value, stats, *end = update(p, sides, now[p], mobility, source, x_halo, z_halo, "last", end)
        stats = gathered(stats)
        *outs, token = scaled(p, 0, field.shape, value, stats, outs)
    inner = [now[1 if late == 0 else top - 1]]
    partial, late_mobility = update(late, inner, now[late], mobility, source, x_halo, z_halo, "partial")
    start = 0
    for side in sent[order[1]]:
        value, stats = finish(start, partial, late_mobility, side, (token,))
        stats = gathered(stats)
        *outs, token = scaled(late, start, field.shape, value, stats, outs)
        end = stored(late, start, field.shape, value, end)
        start += side.shape[0]
    return (*outs, *end)


def solution(mesh):
    spec = P("rows", "cols", "slabs", None)

    return jax.shard_map(per_device, mesh=mesh, in_specs=(spec, spec, spec), out_specs=(spec, spec), check_vma=False)
```
